16 devices in a mesh: dp: 4 (over y, z, core), tp: 4 (over x).
Axes of the slice: x: 4, y: 2, z: 1, core: 2. Of those that a mesh axis runs over, the one named last changes fastest.
The devices are a block of a 4x4x8 slice.
Arguments:
- x: bfloat16 [8192, 7168], P('dp'), parts along dimension 0
- gain: bfloat16 [7168], replicated
- wq: bfloat16 [7168, 7168], P(None, 'tp')
- wk: bfloat16 [7168, 7168], P(None, 'tp')
- wv: bfloat16 [7168, 7168], P(None, 'tp')
- wo: bfloat16 [7168, 7168], P('tp')
Outputs:
- output: bfloat16 [8192, 7168], P('dp'), parts along dimension 0
There are 4 independent parts. The reference program is written for one: setup_inputs(seed, part) draws one part's arguments, and reference() takes and returns one part's arrays. A program takes and returns all parts, laid end to end along the dimension named above; an argument that names none is the same for every part.
All inputs are finite; a program needn't handle non-finite values.
Results may differ from the reference program's by a relative error of at most 0.012.
Values are sent between devices in bfloat16 or wider.
A program may use at most 768 MiB of HBM per device.

```python
import jax
import jax.numpy as jnp
from jax import lax

ROWS = 2048
D = 7168
HEADS = 56
KV_HEADS = 56
HEAD = 128
THETA = 10000


def setup_inputs(seed: int = 0, part: int = 0) -> dict:
    kx, kn, kq, kk, kv, ko = jax.random.split(jax.random.key(seed), 6)

    def weights(key, rows, columns):
        return jax.random.normal(key, (rows, columns), jnp.float32) * rows**-0.5

    drawn = {
        "x": jax.random.normal(jax.random.fold_in(kx, part), (ROWS, D), jnp.float32),
        "gain": 1 + 0.1 * jax.random.normal(kn, (D,), jnp.float32),
        "wq": 2 * weights(kq, D, HEADS * HEAD),
        "wk": 2 * weights(kk, D, KV_HEADS * HEAD),
        "wv": 4 * weights(kv, D, KV_HEADS * HEAD),
        "wo": weights(ko, HEADS * HEAD, D),
    }
    return {k: v.astype(jnp.bfloat16) for k, v in drawn.items()}


def normed(x, gain):
    wide = x.astype(jnp.float32)
    scale = lax.rsqrt(jnp.mean(wide * wide, -1, keepdims=True) + 1e-6)
    return (wide * scale * gain.astype(jnp.float32)).astype(jnp.bfloat16)


def turned(t, place, theta):
    half = t.shape[-1] // 2
    angle = place.astype(jnp.float32)[:, None] * theta ** (-jnp.arange(half, dtype=jnp.float32) / half)
    cos, sin = jnp.cos(angle)[:, None], jnp.sin(angle)[:, None]
    a, b = t[..., :half].astype(jnp.float32), t[..., half:].astype(jnp.float32)
    return jnp.concatenate([a * cos - b * sin, b * cos + a * sin], -1).astype(jnp.bfloat16)


def matmul(a, w):
    return jnp.dot(a, w, preferred_element_type=jnp.float32).astype(jnp.bfloat16)


def einsum(form, a, b):
    return jnp.einsum(form, a.astype(jnp.float32), b.astype(jnp.float32))


def attention(q, k, v):
    scores = einsum("tgsd,ugd->gstu", q, k) * q.shape[-1] ** -0.5
    token = jnp.arange(q.shape[0])
    scores = jnp.where(token[:, None] >= token, scores, -jnp.inf)
    weights = jax.nn.softmax(scores, -1).astype(jnp.bfloat16)
    return einsum("gstu,ugd->tgsd", weights, v).astype(jnp.bfloat16)


def reference(x, gain, wq, wk, wv, wo):
    a, place = normed(x, gain), jnp.arange(ROWS)
    q = turned(matmul(a, wq).reshape(ROWS, HEADS, HEAD), place, THETA).reshape(ROWS, KV_HEADS, -1, HEAD)
    k = turned(matmul(a, wk).reshape(ROWS, KV_HEADS, HEAD), place, THETA)
    v = matmul(a, wv).reshape(ROWS, KV_HEADS, HEAD)
    seen = attention(q, k, v).reshape(ROWS, HEADS * HEAD)
    return (x.astype(jnp.float32) + jnp.dot(seen, wo, preferred_element_type=jnp.float32)).astype(jnp.bfloat16)
```

```python
import functools

import jax
import jax.numpy as jnp
from jax import lax
from jax.experimental import pallas as pl
from jax.experimental.pallas import tpu as pltpu
from jax.sharding import PartitionSpec as P

HEAD = 128
THETA = 10000
EPS = 1e-6
NEG = -1e30
HIDDEN = 2 * NEG
LOG2E = 1.4426950408889634
ROWS = 256
WIDE = 256
SLOTS = 4
GROUP = 7
ONES = 16
LIMIT = 67043328
RING = 4


def _dot(a, b, ca, cb):
    return lax.dot_general(a, b, (((ca,), (cb,)), ((), ())), preferred_element_type=jnp.float32)


def rope_tables(rows):
    half = HEAD // 2
    angle = jnp.arange(rows, dtype=jnp.float32)[:, None] * THETA ** (-jnp.arange(half, dtype=jnp.float32) / half)
    cos, sin = jnp.cos(angle), jnp.sin(angle)
    return jnp.concatenate([cos, cos], -1), jnp.concatenate([-sin, sin], -1)


def _layer(gain, cos_ref, sin_ref, x, wq, wk, wv, wo, y, kc, vt, wbuf, wobuf, xbuf, some, q_s, seen, got, give, acc, done, xres, top_s, mix_s,
           w_sem, wo_sem, x_sem, xres_sem, own_sem, rs_send, rs_recv, ag_send, ag_recv):
    tokens, width = x.shape
    heads = kc.shape[0]
    depth, cols = wobuf.shape[1], wobuf.shape[2]
    chunks = tokens // ROWS
    steps = heads * HEAD // WIDE
    per = WIDE // HEAD
    me = lax.axis_index("tp")
    right, left = lax.rem(me + 1, RING), lax.rem(me + RING - 1, RING)
    to = (right, left)
    scale = HEAD**-0.5 * LOG2E

    barrier = pltpu.get_barrier_semaphore()
    for neighbour in (left, right):
        pl.semaphore_signal(barrier, inc=1, device_id={"tp": neighbour}, device_id_type=pl.DeviceIdType.MESH)

    def rows_of(c):
        return pl.ds(pl.multiple_of(c * ROWS, ROWS), ROWS)

    def cols_of(d, b):
        return pl.ds(pl.multiple_of(d * (width // 2) + lax.rem(b + RING, RING) * cols, 128), cols)

    def tile_copy(kind, j, slot):
        w = (wq, wk, wv)[kind]
        return pltpu.make_async_copy(w.at[:, pl.ds(pl.multiple_of(j * WIDE, WIDE), WIDE)], wbuf.at[slot], w_sem.at[slot])

    def wo_copy(d, hop):
        b = me - 1 - hop if d == 0 else me + 1 + hop
        return pltpu.make_async_copy(wo.at[:, cols_of(d, b)], wobuf.at[d], wo_sem.at[d])

    def x_copy(c):
        return pltpu.make_async_copy(x.at[rows_of(c), :], xbuf, x_sem)

    def xres_copy(d, c):
        return pltpu.make_async_copy(x.at[rows_of(c), cols_of(d, me)], xres.at[d], xres_sem.at[d])

    def own_copy(d, c):
        return pltpu.make_async_copy(done.at[d], y.at[rows_of(c), cols_of(d, me)], own_sem.at[d])

    def sum_copy(d, hop):
        return pltpu.make_async_remote_copy(src_ref=give.at[d, hop], dst_ref=got.at[d, hop], send_sem=rs_send.at[d, hop], recv_sem=rs_recv.at[d, hop],
                                            device_id={"tp": to[d]}, device_id_type=pl.DeviceIdType.MESH)

    def row_copy(d, hop, c):
        place = (rows_of(c), cols_of(d, me - hop if d == 0 else me + hop))
        return pltpu.make_async_remote_copy(src_ref=done.at[d] if hop == 0 else y.at[place], dst_ref=y.at[place], send_sem=ag_send.at[d, hop],
                                            recv_sem=ag_recv.at[d, hop], device_id={"tp": to[d]}, device_id_type=pl.DeviceIdType.MESH)

    def terms(hop, after, c, valid, more):
        for d in range(2):
            wo_copy(d, hop).wait()

            @pl.when(valid)
            def _():
                acc[d] = _dot(seen[lax.rem(c, 2)], wobuf[d], 1, 0)

            @pl.when(more)
            def _():
                wo_copy(d, after).start()

    def add(hop, after, c, valid, more):
        terms(hop, after, c, valid, more)

        @pl.when(valid)
        def _():
            if hop > 0:
                for d in range(2):
                    sum_copy(d, hop - 1).wait_recv()

            @pl.when(c > 0)
            def _():
                for d in range(2):
                    sum_copy(d, hop).wait_send()

            for d in range(2):
                total = acc[d] if hop == 0 else acc[d] + got[d, hop - 1].astype(jnp.float32)
                give[d, hop] = total.astype(jnp.bfloat16)
            for d in range(2):
                sum_copy(d, hop).start()
            if hop == RING - 2:
                for d in range(2):
                    xres_copy(d, c).start()

    def finish(c, valid, more):
        terms(RING - 1, 1, c, valid, more)

        @pl.when(valid)
        def _():
            for d in range(2):
                sum_copy(d, RING - 2).wait_recv()
                xres_copy(d, c).wait()

            @pl.when(c > 0)
            def _():
                for d in range(2):
                    row_copy(d, 0, c).wait_send()
                    own_copy(d, c).wait()
                    row_copy(d, RING - 2, c).wait_recv()

            for d in range(2):
                done[d] = (xres[d].astype(jnp.float32) + (acc[d] + got[d, RING - 2].astype(jnp.float32))).astype(jnp.bfloat16)
            for d in range(2):
                row_copy(d, 0, c).start()
                own_copy(d, c).start()

    def forward(hop, c, valid):
        @pl.when(valid)
        def _():
            for d in range(2):
                row_copy(d, hop - 1, c).wait_recv()

            @pl.when(c > 0)
            def _():
                for d in range(2):
                    row_copy(d, hop, c).wait_send()

            for d in range(2):
                row_copy(d, hop, c).start()

    def norm(p):
        x_copy(p).wait()
        wide_gain = gain[...].astype(jnp.float32)

        def strip(i, _):
            here = pl.ds(pl.multiple_of(i * 16, 16), 16)
            wide = xbuf[here, :].astype(jnp.float32)
            size = lax.rsqrt(jnp.mean(wide * wide, -1, keepdims=True) + EPS)
            some[here, :] = (wide * size * wide_gain).astype(jnp.bfloat16)

        lax.fori_loop(0, ROWS // 16, strip, None)

        @pl.when(p + 1 < chunks)
        def _():
            x_copy(p + 1).start()

    def project(p, j):
        here = rows_of(p)
        for kind in range(3):
            slot = lax.rem((p * steps + j) * 3 + kind, SLOTS)
            tile_copy(kind, j, slot).wait()
            t = _dot(some[...], wbuf[slot], 1, 0).astype(jnp.bfloat16)
            for n in range(per):
                h = j * per + n
                u = t[:, n * HEAD : (n + 1) * HEAD]
                if kind == 2:
                    vt[h, :HEAD, here] = u.T
                else:
                    u = u.astype(jnp.float32)
                    u = (u * cos_ref[here, :] + pltpu.roll(u, HEAD // 2, 1) * sin_ref[here, :]).astype(jnp.bfloat16)
                    if kind == 0:
                        q_s[h] = u
                    else:
                        kc[h, here, :] = u
            ahead, kind_then = divmod(kind + SLOTS, 3)
            then = p * steps + j + ahead

            @pl.when(then < chunks * steps)
            def _():
                tile_copy(kind_then, lax.rem(then, steps), slot).start()

    def attend(p):
        slot = lax.rem(p, 2)

        def group(g, _):
            for n in range(GROUP):
                top_s[n : n + 1, :] = jnp.full((1, ROWS), NEG, jnp.float32)
                mix_s[n] = jnp.zeros((HEAD + ONES, ROWS), jnp.float32)

            def block(b, masked):
                here = rows_of(b)
                scores = [_dot(kc[g * GROUP + n, here, :], q_s[g * GROUP + n], 1, 1) for n in range(GROUP)]
                weights, keeps = [], []
                for n, s in enumerate(scores):
                    if masked:
                        ok = lax.broadcasted_iota(jnp.int32, s.shape, 1) >= lax.broadcasted_iota(jnp.int32, s.shape, 0)
                        s = jnp.where(ok, s, HIDDEN)
                    old = top_s[n : n + 1, :]
                    top = jnp.maximum(old, s.max(axis=0, keepdims=True))
                    top_s[n : n + 1, :] = top
                    weights.append(jnp.exp2((s - top) * scale).astype(jnp.bfloat16))
                    keeps.append(jnp.exp2((old - top) * scale))
                for n, (w, keep) in enumerate(zip(weights, keeps)):
                    mix_s[n] = mix_s[n] * keep + _dot(vt[g * GROUP + n, :, here], w, 1, 0)

            lax.fori_loop(0, p, lambda b, _: block(b, False), None)
            block(p, True)
            for n in range(GROUP):
                out = mix_s[n, :HEAD, :] * (1 / mix_s[n, HEAD : HEAD + 1, :])
                seen[slot, :, pl.ds(pl.multiple_of((g * GROUP + n) * HEAD, HEAD), HEAD)] = out.T.astype(jnp.bfloat16)

        lax.fori_loop(0, heads // GROUP, group, None)

    x_copy(0).start()
    for t in range(SLOTS):
        tile_copy(t % 3, t // 3, t).start()

    def ones(h, _):
        vt[h, HEAD:, :] = jnp.ones((ONES, tokens), jnp.bfloat16)

    lax.fori_loop(0, heads, ones, None)
    pl.semaphore_wait(barrier, 2)
    for d in range(2):
        wo_copy(d, 0).start()

    def period(p, _):
        busy = p < chunks
        new, old = p - 1, p - 2
        summing = (new >= 0) & (new < chunks)
        sending = (old >= 0) & (old < chunks)

        @pl.when(p > 0)
        def _():
            add(0, RING - 1, new, summing, True)

        pl.when(busy)(lambda: norm(p))

        def step(j, _):
            pl.when(busy)(lambda: project(p, j))

            @pl.when((p > 0) & (j == 0))
            def _():
                finish(old, sending, summing)

            @pl.when((p > 0) & (j == 2) & summing)
            def _():
                add(1, 2, new, summing, True)

            pl.when(j == 3)(lambda: forward(1, old, sending))

            @pl.when((p > 0) & (j == 5) & summing)
            def _():
                add(2, 0, new, summing, True)

            pl.when(j == 6)(lambda: forward(2, old, sending))

        lax.fori_loop(0, steps, step, None)
        pl.when(busy)(lambda: attend(p))

    lax.fori_loop(0, chunks + 2, period, None)

    last = chunks - 1
    for d in range(2):
        own_copy(d, last).wait()
        for hop in range(RING - 1):
            sum_copy(d, hop).wait_send()
            row_copy(d, hop, last).wait_send()
        row_copy(d, RING - 2, last).wait_recv()


def solution(mesh):
    def step(x, gain, wq, wk, wv, wo):
        tokens, width = x.shape
        depth = wo.shape[0]
        heads = depth // HEAD
        cols = width // (2 * RING)
        cos, sin = rope_tables(tokens)
        whole, left = pl.BlockSpec(memory_space=pltpu.VMEM), pl.BlockSpec(memory_space=pl.ANY)
        low, full, dma = jnp.bfloat16, jnp.float32, pltpu.SemaphoreType.DMA
        flops = 2 * tokens * width * depth * 4 + 2 * tokens * tokens * depth
        return pl.pallas_call(
            _layer,
            in_specs=[whole] * 3 + [left] * 5,
            out_specs=left,
            out_shape=jax.ShapeDtypeStruct(x.shape, x.dtype),
            scratch_shapes=[
                pltpu.VMEM((heads, tokens, HEAD), low),
                pltpu.VMEM((heads, HEAD + ONES, tokens), low),
                pltpu.VMEM((SLOTS, width, WIDE), low),
                pltpu.VMEM((2, depth, cols), low),
                pltpu.VMEM((ROWS, width), low),
                pltpu.VMEM((ROWS, width), low),
                pltpu.VMEM((heads, ROWS, HEAD), low),
                pltpu.VMEM((2, ROWS, depth), low),
                pltpu.VMEM((2, RING - 1, ROWS, cols), low),
                pltpu.VMEM((2, RING - 1, ROWS, cols), low),
                pltpu.VMEM((2, ROWS, cols), full),
                pltpu.VMEM((2, ROWS, cols), low),
                pltpu.VMEM((2, ROWS, cols), low),
                pltpu.VMEM((GROUP, ROWS), full),
                pltpu.VMEM((GROUP, HEAD + ONES, ROWS), full),
                dma((SLOTS,)),
                dma((2,)),
                dma,
                dma((2,)),
                dma((2,)),
                dma((2, RING - 1)),
                dma((2, RING - 1)),
                dma((2, RING - 1)),
                dma((2, RING - 1)),
            ],
            compiler_params=pltpu.CompilerParams(collective_id=0, has_side_effects=True, vmem_limit_bytes=LIMIT),
            cost_estimate=pl.CostEstimate(flops=flops, transcendentals=tokens * tokens * heads, bytes_accessed=32 * depth * width),
            name="layer",
        )(gain.reshape(1, width), cos, sin, x, wq, wk, wv, wo)

    tokens, columns = P("dp", None), P(None, "tp")
    return jax.shard_map(
        step,
        mesh=mesh,
        in_specs=(tokens, P(None), columns, columns, columns, P("tp", None)),
        out_specs=tokens,
        check_vma=False,
    )
```

```python
import functools

import jax
import jax.numpy as jnp
import numpy as np
from jax import lax
from jax.experimental import pallas as pl
from jax.experimental.pallas import tpu as pltpu
from jax.sharding import PartitionSpec as P

HEAD = 128
THETA = 10000
EPS = 1e-6
NEG = -1e30
HIDDEN = 2 * NEG
LOG2E = 1.4426950408889634
ROWS = 256
DEEP = 1024
PARTS = 2
SLOTS = 4
GROUP = 7
ONES = 16
LIMIT = 67043328
RING = 4
AT = (3, 7, 10, 15, 18)


def _dot(a, b, ca, cb):
    return lax.dot_general(a, b, (((ca,), (cb,)), ((), ())), preferred_element_type=jnp.float32)


def rope_table(rows):
    half = HEAD // 2
    turn = np.float32(THETA) ** (-np.arange(half, dtype=np.float32) / half)
    angle = (np.arange(rows, dtype=np.float32)[:, None] * turn).astype(np.float64)
    return np.concatenate([np.cos(angle), np.sin(angle)], -1).astype(np.float32)


def _layer(gain, table, x, wq, wk, wv, wo, y, kc, vt, wbuf, wobuf, xbuf, some, q_s, seen, got, give, acc, sums, turn_s, done, xres, top_s, mix_s,
           w_sem, wo_sem, x_sem, xres_sem, own_sem, rs_send, rs_recv, ag_send, ag_recv):
    tokens, width = x.shape
    heads = kc.shape[0]
    depth, cols = wobuf.shape[0], wobuf.shape[1] // 2
    chunks = tokens // ROWS
    deep = width // DEEP
    tiles = 3 * deep
    half = slice(0, cols), slice(cols, 2 * cols)
    me = lax.axis_index("tp")
    right, left = lax.rem(me + 1, RING), lax.rem(me + RING - 1, RING)
    to = (right, left)
    scale = HEAD**-0.5 * LOG2E

    barrier = pltpu.get_barrier_semaphore()
    for neighbour in (left, right):
        pl.semaphore_signal(barrier, inc=1, device_id={"tp": neighbour}, device_id_type=pl.DeviceIdType.MESH)

    def rows_of(c):
        return pl.ds(pl.multiple_of(c * ROWS, ROWS), ROWS)

    part_rows = ROWS // PARTS
    parts = range(PARTS)

    def part_of(i):
        return slice(i * part_rows, (i + 1) * part_rows)

    def part_rows_of(c, i):
        return pl.ds(pl.multiple_of(c * ROWS + i * part_rows, part_rows), part_rows)

    def cols_of(d, b):
        return pl.ds(pl.multiple_of(d * (width // 2) + lax.rem(b + RING, RING) * cols, 128), cols)

    def tile_copy(kind, k, slot):
        w = (wq, wk, wv)[kind]
        return pltpu.make_async_copy(w.at[pl.ds(pl.multiple_of(k * DEEP, DEEP), DEEP), :], wbuf.at[slot], w_sem.at[slot])

    def wo_copy(d, hop):
        b = me - 1 - hop if d == 0 else me + 1 + hop
        return pltpu.make_async_copy(wo.at[:, cols_of(d, b)], wobuf.at[:, half[d]], wo_sem.at[d])

    def x_copy(c):
        return pltpu.make_async_copy(x.at[rows_of(c), :], xbuf, x_sem)

    def xres_copy(d, c):
        return pltpu.make_async_copy(x.at[rows_of(c), cols_of(d, me)], xres.at[d], xres_sem.at[d])

    def own_copy(d, c):
        return pltpu.make_async_copy(done.at[d], y.at[rows_of(c), cols_of(d, me)], own_sem.at[d])

    def sum_copy(d, hop, i):
        return pltpu.make_async_remote_copy(src_ref=give.at[d, hop, part_of(i)], dst_ref=got.at[d, hop, part_of(i)], send_sem=rs_send.at[d, hop, i],
                                            recv_sem=rs_recv.at[d, hop, i], device_id={"tp": to[d]}, device_id_type=pl.DeviceIdType.MESH)

    def row_copy(d, hop, c, i):
        place = (part_rows_of(c, i), cols_of(d, me - hop if d == 0 else me + hop))
        return pltpu.make_async_remote_copy(src_ref=done.at[d, part_of(i)] if hop == 0 else y.at[place], dst_ref=y.at[place],
                                            send_sem=ag_send.at[d, hop, i], recv_sem=ag_recv.at[d, hop, i], device_id={"tp": to[d]},
                                            device_id_type=pl.DeviceIdType.MESH)

    def terms(hop, after, c, valid):
        for d in range(2):
            wo_copy(d, hop).wait()

        @pl.when(valid)
        def _():
            acc[...] = _dot(seen[lax.rem(c, 2)], wobuf[...], 1, 0)

        for more, then in after:

            @pl.when(more)
            def _():
                for d in range(2):
                    wo_copy(d, then).start()

    def add(hop, after, c, valid):
        terms(hop, after, c, valid)

        @pl.when(valid)
        def _():
            @pl.when(c > 0)
            def _():
                for d in range(2):
                    for i in parts:
                        sum_copy(d, hop, i).wait_send()

            for i in parts:
                here = part_of(i)
                if hop > 0:
                    for d in range(2):
                        sum_copy(d, hop - 1, i).wait_recv()
                for d in range(2):
                    total = acc[here, half[d]] if hop == 0 else acc[here, half[d]] + got[d, hop - 1, here].astype(jnp.float32)
                    give[d, hop, here] = total.astype(jnp.bfloat16)
                for d in range(2):
                    sum_copy(d, hop, i).start()
            if hop == RING - 2:
                for d in range(2):
                    xres_copy(d, c).start()

    def finish(after, c, valid):
        terms(RING - 1, after, c, valid)

        @pl.when(valid)
        def _():
            for d in range(2):
                xres_copy(d, c).wait()

            @pl.when(c > 0)
            def _():
                for d in range(2):
                    own_copy(d, c).wait()
                    for i in parts:
                        row_copy(d, 0, c, i).wait_send()
                        row_copy(d, RING - 2, c, i).wait_recv()

            for i in parts:
                here = part_of(i)
                for d in range(2):
                    sum_copy(d, RING - 2, i).wait_recv()
                for d in range(2):
                    total = acc[here, half[d]] + got[d, RING - 2, here].astype(jnp.float32)
                    done[d, here] = (xres[d, here].astype(jnp.float32) + total).astype(jnp.bfloat16)
                for d in range(2):
                    row_copy(d, 0, c, i).start()
            for d in range(2):
                own_copy(d, c).start()

    def forward(hop, c, valid):
        @pl.when(valid)
        def _():
            @pl.when(c > 0)
            def _():
                for d in range(2):
                    for i in parts:
                        row_copy(d, hop, c, i).wait_send()

            for i in parts:
                for d in range(2):
                    row_copy(d, hop - 1, c, i).wait_recv()
                for d in range(2):
                    row_copy(d, hop, c, i).start()

    def norm(p):
        x_copy(p).wait()
        wide_gain = gain[...].astype(jnp.float32).reshape(1, width)
        both = table[rows_of(p), :]
        other = pltpu.roll(both, HEAD // 2, 1)
        low = lax.broadcasted_iota(jnp.int32, both.shape, 1) < HEAD // 2
        turn_s[0] = jnp.where(low, both, other)
        turn_s[1] = jnp.where(low, -other, both)

        def strip(i, _):
            here = pl.ds(pl.multiple_of(i * 16, 16), 16)
            wide = xbuf[here, :].astype(jnp.float32)
            size = lax.rsqrt(jnp.mean(wide * wide, -1, keepdims=True) + EPS)
            some[here, :] = (wide * size * wide_gain).astype(jnp.bfloat16)

        lax.fori_loop(0, ROWS // 16, strip, None)

        @pl.when(p + 1 < chunks)
        def _():
            x_copy(p + 1).start()

    def project(p, t):
        at = p * tiles + t
        slot, k = lax.rem(at, SLOTS), lax.rem(t, deep)
        tile_copy(0, k, slot).wait()
        sums[...] += _dot(some[:, pl.ds(pl.multiple_of(k * DEEP, DEEP), DEEP)], wbuf[slot], 1, 0)
        then = at + SLOTS
        next_t = lax.rem(then, tiles)
        for kind in range(3):

            @pl.when((then < chunks * tiles) & (next_t // deep == kind))
            def _():
                tile_copy(kind, lax.rem(next_t, deep), slot).start()

            @pl.when(t == kind * deep + deep - 1)
            def _():
                for h in range(heads):
                    place = slice(h * HEAD, (h + 1) * HEAD)
                    u = sums[:, place].astype(jnp.bfloat16)
                    sums[:, place] = jnp.zeros((ROWS, HEAD), jnp.float32)
                    if kind == 2:
                        vt[h, :HEAD, rows_of(p)] = u.T
                    else:
                        u = u.astype(jnp.float32)
                        u = (u * turn_s[0] + pltpu.roll(u, HEAD // 2, 1) * turn_s[1]).astype(jnp.bfloat16)
                        if kind == 0:
                            q_s[h] = u
                        else:
                            kc[h, rows_of(p), :] = u

    def attend(p):
        slot = lax.rem(p, 2)

        def group(g, _):
            for n in range(GROUP):
                top_s[n : n + 1, :] = jnp.full((1, ROWS), NEG, jnp.float32)
                mix_s[n] = jnp.zeros((HEAD + ONES, ROWS), jnp.float32)

            def block(b, masked):
                here = rows_of(b)
                scores = [_dot(kc[g * GROUP + n, here, :], q_s[g * GROUP + n], 1, 1) for n in range(GROUP)]
                weights, keeps = [], []
                for n, s in enumerate(scores):
                    if masked:
                        ok = lax.broadcasted_iota(jnp.int32, s.shape, 1) >= lax.broadcasted_iota(jnp.int32, s.shape, 0)
                        s = jnp.where(ok, s, HIDDEN)
                    old = top_s[n : n + 1, :]
                    top = jnp.maximum(old, s.max(axis=0, keepdims=True))
                    top_s[n : n + 1, :] = top
                    weights.append(jnp.exp2((s - top) * scale).astype(jnp.bfloat16))
                    keeps.append(jnp.exp2((old - top) * scale))
                for n, (w, keep) in enumerate(zip(weights, keeps)):
                    mix_s[n] = mix_s[n] * keep + _dot(vt[g * GROUP + n, :, here], w, 1, 0)

            lax.fori_loop(0, p, lambda b, _: block(b, False), None)
            block(p, True)
            for n in range(GROUP):
                out = mix_s[n, :HEAD, :] * (1 / mix_s[n, HEAD : HEAD + 1, :])
                seen[slot, :, pl.ds(pl.multiple_of((g * GROUP + n) * HEAD, HEAD), HEAD)] = out.T.astype(jnp.bfloat16)

        lax.fori_loop(0, heads // GROUP, group, None)

    x_copy(0).start()
    for t in range(SLOTS):
        tile_copy(0, t, t).start()

    def ones(h, _):
        vt[h, HEAD:, :] = jnp.ones((ONES, tokens), jnp.bfloat16)

    lax.fori_loop(0, heads, ones, None)
    sums[...] = jnp.zeros_like(sums)
    pl.semaphore_wait(barrier, 2)
    for d in range(2):
        wo_copy(d, 0).start()

    def period(p, _):
        busy = p < chunks
        new, old = p - 1, p - 2
        summing = (new >= 0) & (new < chunks)
        sending = (old >= 0) & (old < chunks)

        @pl.when(p > 0)
        def _():
            add(0, ((p <= 2, 1), (p > 2, RING - 1)), new, summing)

        pl.when(busy)(lambda: norm(p))

        def step(t, _):
            pl.when(busy)(lambda: project(p, t))

            @pl.when((p > 2) & (t == AT[0]))
            def _():
                finish(((summing, 1),), old, sending)

            @pl.when((t == AT[1]) & summing)
            def _():
                add(1, ((True, 2),), new, summing)

            pl.when(t == AT[2])(lambda: forward(1, old, sending))

            @pl.when((t == AT[3]) & summing)
            def _():
                add(2, ((p == 1, RING - 1), (p > 1, 0)), new, summing)

            pl.when(t == AT[4])(lambda: forward(2, old, sending))

        lax.fori_loop(0, tiles, step, None)

        @pl.when(p == 1)
        def _():
            finish(((True, 0),), new, summing)

        pl.when(busy)(lambda: attend(p))

    lax.fori_loop(0, chunks + 2, period, None)

    last = chunks - 1
    for d in range(2):
        own_copy(d, last).wait()
        for i in parts:
            for hop in range(RING - 1):
                sum_copy(d, hop, i).wait_send()
                row_copy(d, hop, last, i).wait_send()
            row_copy(d, RING - 2, last, i).wait_recv()


def solution(mesh):
    def step(x, gain, wq, wk, wv, wo):
        tokens, width = x.shape
        depth = wo.shape[0]
        heads = depth // HEAD
        cols = width // (2 * RING)
        whole, left = pl.BlockSpec(memory_space=pltpu.VMEM), pl.BlockSpec(memory_space=pl.ANY)
        low, full, dma = jnp.bfloat16, jnp.float32, pltpu.SemaphoreType.DMA
        flops = 2 * tokens * width * depth * 4 + 2 * tokens * tokens * depth
        return pl.pallas_call(
            _layer,
            in_specs=[whole] * 2 + [left] * 5,
            out_specs=left,
            out_shape=jax.ShapeDtypeStruct(x.shape, x.dtype),
            scratch_shapes=[
                pltpu.VMEM((heads, tokens, HEAD), low),
                pltpu.VMEM((heads, HEAD + ONES, tokens), low),
                pltpu.VMEM((SLOTS, DEEP, depth), low),
                pltpu.VMEM((depth, 2 * cols), low),
                pltpu.VMEM((ROWS, width), low),
                pltpu.VMEM((ROWS, width), low),
                pltpu.VMEM((heads, ROWS, HEAD), low),
                pltpu.VMEM((2, ROWS, depth), low),
                pltpu.VMEM((2, RING - 1, ROWS, cols), low),
                pltpu.VMEM((2, RING - 1, ROWS, cols), low),
                pltpu.VMEM((ROWS, 2 * cols), full),
                pltpu.VMEM((ROWS, depth), full),
                pltpu.VMEM((2, ROWS, HEAD), full),
                pltpu.VMEM((2, ROWS, cols), low),
                pltpu.VMEM((2, ROWS, cols), low),
                pltpu.VMEM((GROUP, ROWS), full),
                pltpu.VMEM((GROUP, HEAD + ONES, ROWS), full),
                dma((SLOTS,)),
                dma((2,)),
                dma,
                dma((2,)),
                dma((2,)),
                dma((2, RING - 1, PARTS)),
                dma((2, RING - 1, PARTS)),
                dma((2, RING - 1, PARTS)),
                dma((2, RING - 1, PARTS)),
            ],
            compiler_params=pltpu.CompilerParams(collective_id=0, has_side_effects=True, vmem_limit_bytes=LIMIT),
            cost_estimate=pl.CostEstimate(flops=flops, transcendentals=tokens * tokens * heads, bytes_accessed=32 * depth * width),
            name="layer",
        )(gain, jnp.asarray(rope_table(tokens)), x, wq, wk, wv, wo)

    tokens, columns = P("dp", None), P(None, "tp")
    return jax.shard_map(
        step,
        mesh=mesh,
        in_specs=(tokens, P(None), columns, columns, columns, P("tp", None)),
        out_specs=tokens,
        check_vma=False,
    )
```

```python
import functools

import jax
import jax.numpy as jnp
import numpy as np
from jax import lax
from jax.experimental import pallas as pl
from jax.experimental.pallas import tpu as pltpu
from jax.sharding import PartitionSpec as P

HEAD = 128
THETA = 10000
EPS = 1e-6
NEG = -1e30
HIDDEN = 2 * NEG
LOG2E = 1.4426950408889634
ROWS = 256
DEEP = 1024
PARTS = 2
SLOTS = 4
GROUP = 7
ONES = 16
LIMIT = 67043328
RING = 4
AT = (3, 7, 10, 15, 18)


def _dot(a, b, ca, cb):
    return lax.dot_general(a, b, (((ca,), (cb,)), ((), ())), preferred_element_type=jnp.float32)


def rope_table(rows):
    half = HEAD // 2
    turn = np.float32(THETA) ** (-np.arange(half, dtype=np.float32) / half)
    angle = (np.arange(rows, dtype=np.float32)[:, None] * turn).astype(np.float64)
    return np.concatenate([np.cos(angle), np.sin(angle)], -1).astype(np.float32)


def _layer(gain, table, x, wq, wk, wv, wo, y, kc, vt, wbuf, wobuf, xbuf, some, q_s, seen, got, give, acc, sums, turn_s, done, xres, top_s, mix_s,
           w_sem, wo_sem, x_sem, xres_sem, own_sem, rs_send, rs_recv, ag_send, ag_recv):
    tokens, width = x.shape
    heads = kc.shape[0]
    depth, cols = wobuf.shape[0], wobuf.shape[1] // 2
    chunks = tokens // ROWS
    deep = width // DEEP
    tiles = 3 * deep
    half = slice(0, cols), slice(cols, 2 * cols)
    me = lax.axis_index("tp")
    right, left = lax.rem(me + 1, RING), lax.rem(me + RING - 1, RING)
    to = (right, left)
    scale = HEAD**-0.5 * LOG2E

    barrier = pltpu.get_barrier_semaphore()
    for neighbour in (left, right):
        pl.semaphore_signal(barrier, inc=1, device_id={"tp": neighbour}, device_id_type=pl.DeviceIdType.MESH)

    def rows_of(c):
        return pl.ds(pl.multiple_of(c * ROWS, ROWS), ROWS)

    part_rows = ROWS // PARTS
    parts = range(PARTS)

    def part_of(i):
        return slice(i * part_rows, (i + 1) * part_rows)

    def part_rows_of(c, i):
        return pl.ds(pl.multiple_of(c * ROWS + i * part_rows, part_rows), part_rows)

    def cols_of(d, b):
        return pl.ds(pl.multiple_of(d * (width // 2) + lax.rem(b + RING, RING) * cols, 128), cols)

    def tile_copy(kind, k, slot):
        w = (wq, wk, wv)[kind]
        return pltpu.make_async_copy(w.at[pl.ds(pl.multiple_of(k * DEEP, DEEP), DEEP), :], wbuf.at[slot], w_sem.at[slot])

    def wo_copy(d, hop):
        b = me - 1 - hop if d == 0 else me + 1 + hop
        return pltpu.make_async_copy(wo.at[:, cols_of(d, b)], wobuf.at[:, half[d]], wo_sem.at[d])

    def x_copy(c):
        return pltpu.make_async_copy(x.at[rows_of(c), :], xbuf, x_sem)

    def xres_copy(d, c):
        return pltpu.make_async_copy(x.at[rows_of(c), cols_of(d, me)], xres.at[d], xres_sem.at[d])

    def own_copy(d, c):
        return pltpu.make_async_copy(done.at[d], y.at[rows_of(c), cols_of(d, me)], own_sem.at[d])

    def sum_copy(d, hop, i):
        return pltpu.make_async_remote_copy(src_ref=give.at[d, hop, part_of(i)], dst_ref=got.at[d, hop, part_of(i)], send_sem=rs_send.at[d, hop, i],
                                            recv_sem=rs_recv.at[d, hop, i], device_id={"tp": to[d]}, device_id_type=pl.DeviceIdType.MESH)

    def row_copy(d, hop, c, i):
        place = (part_rows_of(c, i), cols_of(d, me - hop if d == 0 else me + hop))
        return pltpu.make_async_remote_copy(src_ref=done.at[d, part_of(i)] if hop == 0 else y.at[place], dst_ref=y.at[place],
                                            send_sem=ag_send.at[d, hop, i], recv_sem=ag_recv.at[d, hop, i], device_id={"tp": to[d]},
                                            device_id_type=pl.DeviceIdType.MESH)

    def terms(hop, after, c, valid):
        for d in range(2):
            wo_copy(d, hop).wait()

        @pl.when(valid)
        def _():
            acc[...] = _dot(seen[lax.rem(c, 2)], wobuf[...], 1, 0)

        for more, then in after:

            @pl.when(more)
            def _():
                for d in range(2):
                    wo_copy(d, then).start()

    def add(hop, after, c, valid):
        terms(hop, after, c, valid)

        @pl.when(valid)
        def _():
            @pl.when(c > 0)
            def _():
                for d in range(2):
                    for i in parts:
                        sum_copy(d, hop, i).wait_send()

            for i in parts:
                here = part_of(i)
                if hop > 0:
                    for d in range(2):
                        sum_copy(d, hop - 1, i).wait_recv()
                for d in range(2):
                    total = acc[here, half[d]] if hop == 0 else acc[here, half[d]] + got[d, hop - 1, here].astype(jnp.float32)
                    give[d, hop, here] = total.astype(jnp.bfloat16)
                for d in range(2):
                    sum_copy(d, hop, i).start()
            if hop == RING - 2:
                for d in range(2):
                    xres_copy(d, c).start()

    def finish(after, c, valid):
        terms(RING - 1, after, c, valid)

        @pl.when(valid)
        def _():
            for d in range(2):
                xres_copy(d, c).wait()

            @pl.when(c > 0)
            def _():
                for d in range(2):
                    own_copy(d, c).wait()
                    for i in parts:
                        row_copy(d, 0, c, i).wait_send()
                        row_copy(d, RING - 2, c, i).wait_recv()

            for i in parts:
                here = part_of(i)
                for d in range(2):
                    sum_copy(d, RING - 2, i).wait_recv()
                for d in range(2):
                    total = acc[here, half[d]] + got[d, RING - 2, here].astype(jnp.float32)
                    done[d, here] = (xres[d, here].astype(jnp.float32) + total).astype(jnp.bfloat16)
                for d in range(2):
                    row_copy(d, 0, c, i).start()
            for d in range(2):
                own_copy(d, c).start()

    def forward(hop, c, valid):
        @pl.when(valid)
        def _():
            @pl.when(c > 0)
            def _():
                for d in range(2):
                    for i in parts:
                        row_copy(d, hop, c, i).wait_send()

            for i in parts:
                for d in range(2):
                    row_copy(d, hop - 1, c, i).wait_recv()
                for d in range(2):
                    row_copy(d, hop, c, i).start()

    def norm(p):
        x_copy(p).wait()

        @pl.when(p == 0)
        def _():
            for t in range(1, SLOTS):
                tile_copy(0, t, t).start()

        wide_gain = gain[...].astype(jnp.float32).reshape(1, width)
        both = table[rows_of(p), :]
        other = pltpu.roll(both, HEAD // 2, 1)
        low = lax.broadcasted_iota(jnp.int32, both.shape, 1) < HEAD // 2
        turn_s[0] = jnp.where(low, both, other)
        turn_s[1] = jnp.where(low, -other, both)

        def strip(i, _):
            here = pl.ds(pl.multiple_of(i * 16, 16), 16)
            wide = xbuf[here, :].astype(jnp.float32)
            size = lax.rsqrt(jnp.mean(wide * wide, -1, keepdims=True) + EPS)
            some[here, :] = (wide * size * wide_gain).astype(jnp.bfloat16)

        lax.fori_loop(0, ROWS // 16, strip, None)

        @pl.when(p + 1 < chunks)
        def _():
            x_copy(p + 1).start()

    def project(p, t):
        at = p * tiles + t
        slot, k = lax.rem(at, SLOTS), lax.rem(t, deep)
        tile_copy(0, k, slot).wait()
        sums[...] += _dot(some[:, pl.ds(pl.multiple_of(k * DEEP, DEEP), DEEP)], wbuf[slot], 1, 0)
        then = at + SLOTS
        next_t = lax.rem(then, tiles)
        for kind in range(3):

            @pl.when((then < chunks * tiles) & (next_t // deep == kind))
            def _():
                tile_copy(kind, lax.rem(next_t, deep), slot).start()

            @pl.when(t == kind * deep + deep - 1)
            def _():
                for h in range(heads):
                    place = slice(h * HEAD, (h + 1) * HEAD)
                    u = sums[:, place].astype(jnp.bfloat16)
                    sums[:, place] = jnp.zeros((ROWS, HEAD), jnp.float32)
                    if kind == 2:
                        vt[h, :HEAD, rows_of(p)] = u.T
                    else:
                        u = u.astype(jnp.float32)
                        u = (u * turn_s[0] + pltpu.roll(u, HEAD // 2, 1) * turn_s[1]).astype(jnp.bfloat16)
                        if kind == 0:
                            q_s[h] = u
                        else:
                            kc[h, rows_of(p), :] = u

    def attend(p):
        slot = lax.rem(p, 2)

        def group(g, _):
            for n in range(GROUP):
                top_s[n : n + 1, :] = jnp.full((1, ROWS), NEG, jnp.float32)
                mix_s[n] = jnp.zeros((HEAD + ONES, ROWS), jnp.float32)

            def block(b, masked):
                here = rows_of(b)
                scores = [_dot(kc[g * GROUP + n, here, :], q_s[g * GROUP + n], 1, 1) for n in range(GROUP)]
                weights, keeps = [], []
                for n, s in enumerate(scores):
                    if masked:
                        ok = lax.broadcasted_iota(jnp.int32, s.shape, 1) >= lax.broadcasted_iota(jnp.int32, s.shape, 0)
                        s = jnp.where(ok, s, HIDDEN)
                    old = top_s[n : n + 1, :]
                    top = jnp.maximum(old, s.max(axis=0, keepdims=True))
                    top_s[n : n + 1, :] = top
                    weights.append(jnp.exp2((s - top) * scale).astype(jnp.bfloat16))
                    keeps.append(jnp.exp2((old - top) * scale))
                for n, (w, keep) in enumerate(zip(weights, keeps)):
                    mix_s[n] = mix_s[n] * keep + _dot(vt[g * GROUP + n, :, here], w, 1, 0)

            lax.fori_loop(0, p, lambda b, _: block(b, False), None)
            block(p, True)
            for n in range(GROUP):
                out = mix_s[n, :HEAD, :] * (1 / mix_s[n, HEAD : HEAD + 1, :])
                seen[slot, :, pl.ds(pl.multiple_of((g * GROUP + n) * HEAD, HEAD), HEAD)] = out.T.astype(jnp.bfloat16)

        lax.fori_loop(0, heads // GROUP, group, None)

    x_copy(0).start()
    tile_copy(0, 0, 0).start()

    def ones(h, _):
        vt[h, HEAD:, :] = jnp.ones((ONES, tokens), jnp.bfloat16)

    lax.fori_loop(0, heads, ones, None)
    sums[...] = jnp.zeros_like(sums)
    pl.semaphore_wait(barrier, 2)

    def period(p, _):
        busy = p < chunks
        new, old = p - 1, p - 2
        summing = (new >= 0) & (new < chunks)
        sending = (old >= 0) & (old < chunks)

        @pl.when(p > 0)
        def _():
            add(0, ((p <= 2, 1), (p > 2, RING - 1)), new, summing)

        pl.when(busy)(lambda: norm(p))

        def step(t, _):
            pl.when(busy)(lambda: project(p, t))

            @pl.when((p == 0) & (t == tiles // 2))
            def _():
                for d in range(2):
                    wo_copy(d, 0).start()

            @pl.when((p > 2) & (t == AT[0]))
            def _():
                finish(((summing, 1),), old, sending)

            @pl.when((t == AT[1]) & summing)
            def _():
                add(1, ((True, 2),), new, summing)

            pl.when(t == AT[2])(lambda: forward(1, old, sending))

            @pl.when((t == AT[3]) & summing)
            def _():
                add(2, ((p == 1, RING - 1), (p > 1, 0)), new, summing)

            pl.when(t == AT[4])(lambda: forward(2, old, sending))

        lax.fori_loop(0, tiles, step, None)

        @pl.when(p == 1)
        def _():
            finish(((True, 0),), new, summing)

        pl.when(busy)(lambda: attend(p))

    lax.fori_loop(0, chunks + 2, period, None)

    last = chunks - 1
    for d in range(2):
        own_copy(d, last).wait()
        for i in parts:
            for hop in range(RING - 1):
                sum_copy(d, hop, i).wait_send()
                row_copy(d, hop, last, i).wait_send()
            row_copy(d, RING - 2, last, i).wait_recv()


def solution(mesh):
    def step(x, gain, wq, wk, wv, wo):
        tokens, width = x.shape
        depth = wo.shape[0]
        heads = depth // HEAD
        cols = width // (2 * RING)
        whole, left = pl.BlockSpec(memory_space=pltpu.VMEM), pl.BlockSpec(memory_space=pl.ANY)
        low, full, dma = jnp.bfloat16, jnp.float32, pltpu.SemaphoreType.DMA
        flops = 2 * tokens * width * depth * 4 + 2 * tokens * tokens * depth
        return pl.pallas_call(
            _layer,
            in_specs=[whole] * 2 + [left] * 5,
            out_specs=left,
            out_shape=jax.ShapeDtypeStruct(x.shape, x.dtype),
            scratch_shapes=[
                pltpu.VMEM((heads, tokens, HEAD), low),
                pltpu.VMEM((heads, HEAD + ONES, tokens), low),
                pltpu.VMEM((SLOTS, DEEP, depth), low),
                pltpu.VMEM((depth, 2 * cols), low),
                pltpu.VMEM((ROWS, width), low),
                pltpu.VMEM((ROWS, width), low),
                pltpu.VMEM((heads, ROWS, HEAD), low),
                pltpu.VMEM((2, ROWS, depth), low),
                pltpu.VMEM((2, RING - 1, ROWS, cols), low),
                pltpu.VMEM((2, RING - 1, ROWS, cols), low),
                pltpu.VMEM((ROWS, 2 * cols), full),
                pltpu.VMEM((ROWS, depth), full),
                pltpu.VMEM((2, ROWS, HEAD), full),
                pltpu.VMEM((2, ROWS, cols), low),
                pltpu.VMEM((2, ROWS, cols), low),
                pltpu.VMEM((GROUP, ROWS), full),
                pltpu.VMEM((GROUP, HEAD + ONES, ROWS), full),
                dma((SLOTS,)),
                dma((2,)),
                dma,
                dma((2,)),
                dma((2,)),
                dma((2, RING - 1, PARTS)),
                dma((2, RING - 1, PARTS)),
                dma((2, RING - 1, PARTS)),
                dma((2, RING - 1, PARTS)),
            ],
            compiler_params=pltpu.CompilerParams(collective_id=0, has_side_effects=True, vmem_limit_bytes=LIMIT),
            cost_estimate=pl.CostEstimate(flops=flops, transcendentals=tokens * tokens * heads, bytes_accessed=32 * depth * width),
            name="layer",
        )(gain, jnp.asarray(rope_table(tokens)), x, wq, wk, wv, wo)

    tokens, columns = P("dp", None), P(None, "tp")
    return jax.shard_map(
        step,
        mesh=mesh,
        in_specs=(tokens, P(None), columns, columns, columns, P("tp", None)),
        out_specs=tokens,
        check_vma=False,
    )
```
